512 devices in a mesh: batch: 64 (over y, z), table: 8 (over x, core).
Axes of the slice: x: 4, y: 4, z: 16, core: 2. Of those that a mesh axis runs over, the one named last changes fastest.
Arguments:
- embeddings: bfloat16 [64, 2048, 128], P('table'), may hold values from -0.59765625 to 0.59765625
- feature_ids: int32 [65536, 512], P('batch', 'table'), may hold values from 0 to 2047
- counts: int32 [65536, 64], P('batch', 'table'), may hold values from 0 to 8, as said below
Outputs:
- gram: bfloat16 [65536, 4096], P(('batch', 'table'))
- offsets: int32 [65536], P(('batch', 'table'))
The draws below stay inside these ranges and needn't reach their ends.
Inputs may be any that keep to these rules, and one draw needn't show every extreme that they name: `counts`: the value 8 occurs in every device's block.
All inputs are finite; a program needn't handle non-finite values.
Results may differ from the reference program's by a relative error of at most 0.001.
The reference program's roundings to bfloat16 on the way (of `pooled`) count: a program that leaves them out, or rounds other values in their place, can miss the bound.
Values may be sent and summed in bfloat16 or wider, within the bound.
A program may use at most 64 MiB of HBM per device.

```python
import jax
import jax.numpy as jnp
from jax import lax

E = 128
F = 64
MAXF = 8
V = 2048
B_DEV = 1024
TOKENS = 65536


def draw_counts(key, part):
    first = jax.random.fold_in(key, 11)
    second = jax.random.fold_in(key, 23)
    rows = jnp.arange(TOKENS, dtype=jnp.int32)[:, None]
    cols = jnp.arange(F, dtype=jnp.int32)[None, :]
    live = jax.random.randint(first, (TOKENS, F), 0, 3 * TOKENS) < TOKENS + 2 * rows
    value = jax.random.randint(second, (TOKENS, F), 1, MAXF + 1)
    forced = (rows * F + cols) % 97 == 0
    return jnp.where(forced, MAXF, jnp.where(live, value, 0)).astype(jnp.int32)


def touch_ends(values, rng, low, largest):
    spot = [jax.random.randint(jax.random.fold_in(rng, axis), (), 0, length) for axis, length in enumerate(values.shape)]
    main_axis = values.shape.index(max(values.shape))
    beside = spot[:main_axis] + [(spot[main_axis] + 1) % values.shape[main_axis]] + spot[main_axis + 1:]
    return values.at[tuple(spot)].set(low).at[tuple(beside)].set(largest)


def block_levels(stream_key, dims, pieces, least, largest):
    level, own = 1.0, jax.random.fold_in(stream_key, 6)
    for position, shards_of in pieces:
        heights = jnp.exp(jax.random.uniform(jax.random.fold_in(own, position), (shards_of,), jnp.float32, least / len(pieces), largest / len(pieces)))
        level = level * jnp.repeat(heights, dims[position] // shards_of).reshape([-1 if axis == position else 1 for axis in range(len(dims))])
    return level


def normal_values(stream_key, dims, deviation, reach, shards=(), kind=jnp.bfloat16):
    drawn = jax.random.normal(stream_key, dims, jnp.float32) * deviation
    if len(shards) > 0:
        drawn = block_levels(stream_key, dims, shards, -0.22, 0.18) * drawn
    return jnp.clip(drawn, min=-reach, max=reach).astype(kind)


def setup_inputs(seed: int = 0) -> dict:
    key_list = jax.random.split(jax.random.key(seed), 4)
    return {
        "embeddings": normal_values(key_list[0], (F, V, E), 0.1, 0.59765625, ((0, 8),)),
        "feature_ids": touch_ends(jax.random.randint(key_list[1], (TOKENS, F * MAXF), 0, V), jax.random.fold_in(key_list[1], 1), 0, V - 1).astype(jnp.int32),
        "counts": draw_counts(jax.random.fold_in(key_list[3], 71), 0),
    }


def pool_one(table, idents, number):
    rows = jnp.take(table, idents, axis=0).astype(jnp.float32)
    slots = jnp.arange(MAXF, dtype=jnp.int32)[None, :]
    keep = (slots < number[:, None]).astype(jnp.float32)
    return jnp.sum(rows * keep[:, :, None], axis=1)


def reference(embeddings, feature_ids, counts):
    idents = feature_ids.reshape(TOKENS, F, MAXF).transpose(1, 0, 2)
    pooled = lax.map(lambda a: pool_one(a[0], a[1], a[2]), (embeddings, idents, counts.T))
    pooled = pooled.transpose(1, 0, 2).astype(jnp.bfloat16)
    blocks = pooled.reshape(TOKENS // B_DEV, B_DEV, F, E)

    def block_gram(part):
        wide = part.astype(jnp.float32)
        return jnp.einsum("sie,sje->sij", wide, wide).astype(jnp.bfloat16).reshape(B_DEV, F * F)

    gram = lax.map(block_gram, blocks).reshape(TOKENS, F * F)
    live = jnp.sum((counts > 0).astype(jnp.int32), axis=1)
    pairs = live * (live - 1) // 2
    offsets = (jnp.cumsum(pairs) - pairs).astype(jnp.int32)
    return gram, offsets
```

```python
import jax
import jax.numpy as jnp
from jax import lax
from jax.experimental import pallas as pl
from jax.experimental.pallas import tpu as pltpu
from jax.sharding import PartitionSpec as P

BF = jnp.bfloat16
F32 = jnp.float32
I32 = jnp.int32
MESH = pl.DeviceIdType.MESH
MAXF = 8
NT = 8
NK = 8
NY, NZ = 4, 16
LANES = 128
TRI = (((1,), (1,)), ((), ()))


def make_keys(ids, cnt, ka, kb):
    lane = lax.broadcasted_iota(I32, (8, LANES), 1)
    sub = lax.broadcasted_iota(I32, (8, LANES), 0)
    place = [jnp.logical_and((sub & 3) == b, (lane >> 5) == b) for b in range(4)]

    def tile(q, carry):
        c0 = pl.multiple_of(q * LANES, LANES)
        for t in range(NT):
            v = ids[t * 8 : t * 8 + 8, pl.ds(c0, LANES)]
            v = jnp.where(sub >= cnt[t : t + 1, pl.ds(c0, LANES)], 2048, v)
            turned = [v] + [pltpu.roll(v, 32 * k, 1) for k in range(1, 4)]
            for a in range(4):
                m = jnp.zeros_like(v)
                for b in range(4):
                    m = jnp.where(place[b], turned[(b - a) % 4], m)
                m = m + pltpu.roll(m, 7, 0)
                m = m + pltpu.roll(m, 6, 0)
                za = (((m >> 8) << 5) + (lane & 31)).astype(F32)
                zb = (m & 255).astype(F32)
                for h in range(2):
                    ka[q, t, a : a + 1, h * 128 : h * 128 + 128] = za[4 * h : 4 * h + 1, :]
                    kb[q, t, a : a + 1, h * 128 : h * 128 + 128] = zb[4 * h : 4 * h + 1, :]
        return carry

    lax.fori_loop(0, 8, tile, 0)


def pool_body(ids, cnt, tab_hbm, out, offs, tab, ka, kb, iota, w, stage, sb, lv, lvall, tot, ztot, yline,
              tsem, ssem, rsem, lsem, lss, lrs, zss, zrs, yss, yrs):
    b, k = lax.axis_index("batch"), lax.axis_index("table")
    y, z = b // NZ, b % NZ
    x, c = k // 2, k % 2

    bar = pltpu.get_barrier_semaphore()
    for d in range(1, NK):
        pl.semaphore_signal(bar, inc=1, device_id=(b, (k + d) % NK), device_id_type=MESH)
    for d in range(1, NZ):
        pl.semaphore_signal(bar, inc=1, device_id=(y * NZ + (z + d) % NZ, k), device_id_type=MESH)
    for d in range(1, NY):
        pl.semaphore_signal(bar, inc=1, device_id=(((y + d) % NY) * NZ + z, k), device_id_type=MESH)

    def table_copy(t):
        return pltpu.make_async_copy(tab_hbm.at[t], tab.at[t], tsem.at[t])

    for t in range(NT):
        table_copy(t).start()

    iota[...] = lax.broadcasted_iota(I32, (256, 256), 0).astype(F32).astype(BF)
    make_keys(ids, cnt, ka, kb)

    for q in range(8):
        on = (cnt[:, q * 128 : q * 128 + 128] > 0).astype(I32)
        lv[q : q + 1, :] = jnp.sum(on, axis=0, keepdims=True)

    def turn(j):
        return (2 + 3 * j + 3 * ((j * (j - 1)) // 2)) % 4

    def chunk_copy(j, cc):
        h, xd = j // 4, (x + turn(j % 4)) % 4
        return pltpu.make_async_remote_copy(
            src_ref=sb.at[j, cc], dst_ref=out.at[h, k], send_sem=ssem.at[j * 2 + cc],
            recv_sem=rsem.at[k * 2 + h], device_id=(b, xd * 2 + cc), device_id_type=MESH)

    def partner_copy(j):
        h = j // 4
        return pltpu.make_async_remote_copy(
            src_ref=sb.at[j, 1 - c], dst_ref=out.at[h, k], send_sem=ssem.at[j * 2],
            recv_sem=rsem.at[k * 2 + h], device_id=(b, x * 2 + 1 - c), device_id_type=MESH)

    def own_copy(j):
        h = j // 4
        return pltpu.make_async_copy(sb.at[j, c], out.at[h, k], lsem.at[h])

    def live_copy(d):
        return pltpu.make_async_remote_copy(
            src_ref=lv, dst_ref=lvall.at[k], send_sem=lss.at[d], recv_sem=lrs.at[k],
            device_id=(b, (k + d) % NK), device_id_type=MESH)

    def z_copy(d):
        return pltpu.make_async_remote_copy(
            src_ref=tot, dst_ref=ztot.at[z], send_sem=zss.at[d], recv_sem=zrs.at[z],
            device_id=(y * NZ + (z + d) % NZ, k), device_id_type=MESH)

    def y_copy(d):
        return pltpu.make_async_remote_copy(
            src_ref=yline.at[y], dst_ref=yline.at[y], send_sem=yss.at[d], recv_sem=yrs.at[y],
            device_id=(((y + d) % NY) * NZ + z, k), device_id_type=MESH)

    def arrival(ref, sem):
        return pltpu.make_async_remote_copy(
            src_ref=ref, dst_ref=ref, send_sem=sem, recv_sem=sem, device_id=(b, k), device_id_type=MESH)

    def rows_of(i):
        j = i // 4
        return j, j // 4, (x + turn(j % 4)) % 4, (i % 4) * 2

    def first(i, slot):
        j, h, xd, t0 = rows_of(i)
        one, zero = jnp.ones((16, 256), BF), jnp.zeros((16, 256), BF)
        for tt in range(2):
            for g in range(4):
                q, a = xd * 2 + g // 2, h * 2 + g % 2
                ra = jnp.broadcast_to(ka[q, t0 + tt, pl.ds(a, 1), :], (16, 256)).astype(BF)
                rb = jnp.broadcast_to(kb[q, t0 + tt, pl.ds(a, 1), :], (16, 256)).astype(BF)
                la, lb = [], []
                for r in range(16):
                    row = iota[r * 16 : r * 16 + 16, :]
                    la.append(jnp.where(row == ra, one, zero))
                    lb.append(jnp.where(row == rb, one, zero))
                n = lax.dot_general(jnp.concatenate(la, 0), jnp.concatenate(lb, 0), TRI,
                                    preferred_element_type=F32).astype(BF)
                for hi in range(8):
                    w[slot, tt, hi, g * 32 : g * 32 + 32, :] = n[hi * 32 : hi * 32 + 32, :]

    def second(i, slot):
        j, h, xd, t0 = rows_of(i)
        for tt in range(2):
            acc = None
            for hi in range(8):
                d = jnp.dot(w[slot, tt, hi], tab[t0 + tt, hi * 256 : hi * 256 + 256, :],
                            preferred_element_type=F32)
                acc = d if acc is None else acc + d
            stage[pl.ds(t0 + tt, 128, 8), :] = acc

    def finish(j):
        for cc in range(2):
            sb[j, cc] = stage[cc * 512 : cc * 512 + 512, :].astype(BF)

        @pl.when(j % 4 < 3)
        def _():
            for cc in range(2):
                chunk_copy(j, cc).start()

        @pl.when(j % 4 == 3)
        def _():
            partner_copy(j).start()
            own_copy(j).start()

    def pairs_of():
        live = lv[...]
        for d in range(1, NK):
            live = live + lvall[(k + d) % NK]
        return (live * (live - 1)) >> 1

    def sum_all(v):
        s = jnp.sum(jnp.sum(v, axis=0, keepdims=True), axis=1, keepdims=True)
        return jnp.broadcast_to(s, (8, LANES))

    def step(i, carry):
        slot = i % 2

        @pl.when(i <= 4)
        def _():
            table_copy((i - 1) * 2).wait()
            table_copy((i - 1) * 2 + 1).wait()

        second(i - 1, 1 - slot)
        first(i, slot)

        @pl.when(i == 4)
        def _():
            pl.semaphore_wait(bar, NK - 1 + NZ - 1 + NY - 1)
            for d in range(1, NK):
                live_copy(d).start()

        @pl.when(i % 4 == 0)
        def _():
            finish(i // 4 - 1)

        @pl.when(i == 9)
        def _():
            for d in range(1, NK):
                arrival(lvall.at[(k + d) % NK], lrs.at[(k + d) % NK]).wait_recv()
            tot[...] = sum_all(pairs_of())
            ztot[z] = tot[...]
            for d in range(1, NZ):
                z_copy(d).start()

        @pl.when(i == 21)
        def _():
            for d in range(1, NZ):
                arrival(ztot.at[(z + d) % NZ], zrs.at[(z + d) % NZ]).wait_recv()
            line = ztot[0]
            for d in range(1, NZ):
                line = line + ztot[d]
            yline[y] = line
            for d in range(1, NY):
                y_copy(d).start()

        return carry

    first(0, 0)
    lax.fori_loop(1, 32, step, 0)
    second(31, 1)
    finish(7)

    for d in range(1, NY):
        arrival(yline.at[(y + d) % NY], yrs.at[(y + d) % NY]).wait_recv()
    lane = lax.broadcasted_iota(I32, (8, LANES), 1)
    sub = lax.broadcasted_iota(I32, (8, LANES), 0)
    before = jnp.zeros((8, LANES), I32)
    for d in range(NY):
        before = before + jnp.where(d < y, yline[d], 0)
    for d in range(NZ):
        before = before + jnp.where(d < z, ztot[d], 0)
    pairs = pairs_of()
    run = pairs
    for n in range(7):
        run = run + jnp.where(lane >= (1 << n), pltpu.roll(run, 1 << n, 1), 0)
    before = before + sum_all(jnp.where(sub < k, pairs, 0))
    mine = jnp.sum(jnp.where(sub == k, run - pairs, 0), axis=0, keepdims=True)
    offs[...] = mine + before[0:1, :]

    for d in range(1, NK):
        live_copy(d).wait_send()
    for d in range(1, NZ):
        z_copy(d).wait_send()
    for d in range(1, NY):
        y_copy(d).wait_send()
    for h in range(2):
        for j in range(3):
            for cc in range(2):
                chunk_copy(h * 4 + j, cc).wait_send()
        partner_copy(h * 4 + 3).wait_send()
        own_copy(h * 4 + 3).wait()
        for d in range(1, NK):
            src = (k + d) % NK
            arrival(out.at[h, src], rsem.at[src * 2 + h]).wait_recv()


def pool_exchange(ids, cnt, tab):
    dma = pltpu.SemaphoreType.DMA
    return pl.pallas_call(
        pool_body,
        out_shape=(jax.ShapeDtypeStruct((2, NK, 512, LANES), BF), jax.ShapeDtypeStruct((1, LANES), I32)),
        in_specs=[pl.BlockSpec(memory_space=pltpu.VMEM)] * 2 + [pl.BlockSpec(memory_space=pl.ANY)],
        out_specs=(pl.BlockSpec(memory_space=pl.ANY), pl.BlockSpec(memory_space=pltpu.VMEM)),
        scratch_shapes=[
            pltpu.VMEM((NT, 2048, LANES), BF),
            pltpu.VMEM((8, NT, 4, 256), F32),
            pltpu.VMEM((8, NT, 4, 256), F32),
            pltpu.VMEM((256, 256), BF),
            pltpu.VMEM((2, 2, 8, 128, 256), BF),
            pltpu.VMEM((1024, LANES), F32),
            pltpu.VMEM((8, 2, 512, LANES), BF),
            pltpu.VMEM((8, LANES), I32),
            pltpu.VMEM((NK, 8, LANES), I32),
            pltpu.VMEM((8, LANES), I32),
            pltpu.VMEM((NZ, 8, LANES), I32),
            pltpu.VMEM((NY, 8, LANES), I32),
            dma((NT,)), dma((16,)), dma((16,)), dma((2,)),
            dma((NK,)), dma((NK,)), dma((NZ,)), dma((NZ,)), dma((NY,)), dma((NY,)),
        ],
        compiler_params=pltpu.CompilerParams(
            collective_id=0, has_side_effects=True, vmem_limit_bytes=40 * 2**20),
        name="pool_exchange",
    )(ids, cnt, tab)


def gram_body(src, out, g):
    low = lax.broadcasted_iota(I32, (16, LANES), 1) < 64
    for half in range(2):
        for p in range(8):
            r0 = half * 128 + p * 16
            got = [src[0, s, r0 : r0 + 16, :].astype(F32) for s in range(NK)]
            even = jnp.concatenate([v[0:8] for v in got], 0).astype(BF)
            odd = jnp.concatenate([v[8:16] for v in got], 0).astype(BF)
            for n, m in ((0, even), (1, odd)):
                full = lax.dot_general(m, jnp.concatenate([m, m], 0), TRI, preferred_element_type=F32)
                g[half, (p * 2 + n) * 64 : (p * 2 + n) * 64 + 64, :] = full
    for half in range(2):
        for i in range(32):
            lo = g[half, pl.ds(2 * i, 16, 64), :]
            hi = g[half, pl.ds(2 * i + 1, 16, 64), :]
            out[half * 16 : half * 16 + 16, i * 128 : i * 128 + 128] = jnp.where(low, lo, hi).astype(BF)


def gram(got):
    return pl.pallas_call(
        gram_body,
        grid=(4,),
        out_shape=jax.ShapeDtypeStruct((128, 4096), BF),
        in_specs=[pl.BlockSpec((1, NK, 256, LANES), lambda i: (i // 2, 0, i % 2, 0))],
        out_specs=pl.BlockSpec((32, 4096), lambda i: (i, 0)),
        scratch_shapes=[pltpu.VMEM((2, 1024, LANES), F32)],
        name="gram",
    )(got)


def body(embeddings, feature_ids, counts):
    got, offsets = pool_exchange(feature_ids.T, counts.T, embeddings)
    return gram(got), offsets.reshape(LANES)


def solution(mesh):
    return jax.shard_map(
        body, mesh=mesh,
        in_specs=(P("table", None, None), P("batch", "table"), P("batch", "table")),
        out_specs=(P(("batch", "table"), None), P(("batch", "table"))),
        check_vma=False)
```

```python
import jax
import jax.numpy as jnp
from jax import lax
from jax.experimental import pallas as pl
from jax.experimental.pallas import tpu as pltpu
from jax.sharding import PartitionSpec as P

BF = jnp.bfloat16
F32 = jnp.float32
I32 = jnp.int32
MESH = pl.DeviceIdType.MESH
MAXF = 8
NT = 8
NK = 8
NY, NZ = 4, 16
LANES = 128
TRI = (((1,), (1,)), ((), ()))


def make_keys(ids, cnt, ka, kb):
    lane = lax.broadcasted_iota(I32, (8, LANES), 1)
    sub = lax.broadcasted_iota(I32, (8, LANES), 0)
    place = [jnp.logical_and((sub & 3) == b, (lane >> 5) == b) for b in range(4)]

    def tile(q, carry):
        c0 = pl.multiple_of(q * LANES, LANES)
        for t in range(NT):
            v = ids[t * 8 : t * 8 + 8, pl.ds(c0, LANES)]
            v = jnp.where(sub >= cnt[t : t + 1, pl.ds(c0, LANES)], 2048, v)
            turned = [v] + [pltpu.roll(v, 32 * k, 1) for k in range(1, 4)]
            for a in range(4):
                m = jnp.zeros_like(v)
                for b in range(4):
                    m = jnp.where(place[b], turned[(b - a) % 4], m)
                m = m + pltpu.roll(m, 7, 0)
                m = m + pltpu.roll(m, 6, 0)
                za = (((m >> 8) << 5) + (lane & 31)).astype(F32)
                zb = (m & 255).astype(F32)
                for h in range(2):
                    ka[q, t, a : a + 1, h * 128 : h * 128 + 128] = za[4 * h : 4 * h + 1, :]
                    kb[q, t, a : a + 1, h * 128 : h * 128 + 128] = zb[4 * h : 4 * h + 1, :]
        return carry

    lax.fori_loop(0, 8, tile, 0)


def pool_body(ids_hbm, cnt_hbm, tab_hbm, out, offs, ids, cnt, tab, ka, kb, iota, w, stage, sb, lv, lvall, tot, ytot, ztot,
              isem, tsem, ssem, rsem, lsem, lss, lrs, zss, zrs, yss, yrs):
    b, k = lax.axis_index("batch"), lax.axis_index("table")
    y, z = b // NZ, b % NZ
    x, c = k // 2, k % 2

    bar = pltpu.get_barrier_semaphore()
    for d in range(1, NK):
        pl.semaphore_signal(bar, inc=1, device_id=(b, (k + d) % NK), device_id_type=MESH)
    for d in range(1, NZ):
        @pl.when(z + d < NZ)
        def _():
            pl.semaphore_signal(bar, inc=1, device_id=(b + d, k), device_id_type=MESH)
    for d in range(1, NY):
        pl.semaphore_signal(bar, inc=1, device_id=(((y + d) % NY) * NZ + z, k), device_id_type=MESH)

    def table_copy(t):
        return pltpu.make_async_copy(tab_hbm.at[t], tab.at[t], tsem.at[t])

    id_copy = pltpu.make_async_copy(ids_hbm, ids, isem.at[0])
    count_copy = pltpu.make_async_copy(cnt_hbm, cnt, isem.at[1])
    id_copy.start()
    count_copy.start()
    for t in range(NT):
        table_copy(t).start()

    iota[...] = lax.broadcasted_iota(I32, (256, 256), 0).astype(F32).astype(BF)
    id_copy.wait()
    count_copy.wait()
    make_keys(ids, cnt, ka, kb)

    for q in range(8):
        on = (cnt[:, q * 128 : q * 128 + 128] > 0).astype(I32)
        lv[q : q + 1, :] = jnp.sum(on, axis=0, keepdims=True)

    def turn(j):
        return (2 + 3 * j + 3 * ((j * (j - 1)) // 2)) % 4

    def chunk_copy(j, cc):
        h, xd = j // 4, (x + turn(j % 4)) % 4
        return pltpu.make_async_remote_copy(
            src_ref=sb.at[j, cc], dst_ref=out.at[h, k], send_sem=ssem.at[j * 2 + cc],
            recv_sem=rsem.at[k * 2 + h], device_id=(b, xd * 2 + cc), device_id_type=MESH)

    def partner_copy(j):
        h = j // 4
        return pltpu.make_async_remote_copy(
            src_ref=sb.at[j, 1 - c], dst_ref=out.at[h, k], send_sem=ssem.at[j * 2],
            recv_sem=rsem.at[k * 2 + h], device_id=(b, x * 2 + 1 - c), device_id_type=MESH)

    def own_copy(j):
        h = j // 4
        return pltpu.make_async_copy(sb.at[j, c], out.at[h, k], lsem.at[h])

    def live_copy(d):
        return pltpu.make_async_remote_copy(
            src_ref=lv, dst_ref=lvall.at[k], send_sem=lss.at[d], recv_sem=lrs.at[k],
            device_id=(b, (k + d) % NK), device_id_type=MESH)

    def y_copy(d):
        return pltpu.make_async_remote_copy(
            src_ref=tot, dst_ref=ytot.at[y], send_sem=yss.at[d], recv_sem=yrs.at[y],
            device_id=(((y + d) % NY) * NZ + z, k), device_id_type=MESH)

    def z_copy(d):
        return pltpu.make_async_remote_copy(
            src_ref=ztot.at[z], dst_ref=ztot.at[z], send_sem=zss.at[d + NZ], recv_sem=zrs.at[z],
            device_id=(b + d, k), device_id_type=MESH)

    def z_arrival(d):
        return arrival(ztot.at[z + d], zrs.at[z + d])

    def reply(lo, hi):
        for d in range(lo, hi):
            @pl.when(z + d < NZ)
            def _():
                z_arrival(d).wait_recv()
                z_copy(d).start()

    def arrival(ref, sem):
        return pltpu.make_async_remote_copy(
            src_ref=ref, dst_ref=ref, send_sem=sem, recv_sem=sem, device_id=(b, k), device_id_type=MESH)

    def rows_of(i):
        j = i // 4
        return j, j // 4, (x + turn(j % 4)) % 4, (i % 4) * 2

    def first(i, slot):
        j, h, xd, t0 = rows_of(i)
        one, zero = jnp.ones((16, 256), BF), jnp.zeros((16, 256), BF)
        for tt in range(2):
            for g in range(4):
                q, a = xd * 2 + g // 2, h * 2 + g % 2
                ra = jnp.broadcast_to(ka[q, t0 + tt, pl.ds(a, 1), :], (16, 256)).astype(BF)
                rb = jnp.broadcast_to(kb[q, t0 + tt, pl.ds(a, 1), :], (16, 256)).astype(BF)
                la, lb = [], []
                for r in range(16):
                    row = iota[r * 16 : r * 16 + 16, :]
                    la.append(jnp.where(row == ra, one, zero))
                    lb.append(jnp.where(row == rb, one, zero))
                n = lax.dot_general(jnp.concatenate(la, 0), jnp.concatenate(lb, 0), TRI,
                                    preferred_element_type=F32).astype(BF)
                for hi in range(8):
                    w[slot, tt, hi, g * 32 : g * 32 + 32, :] = n[hi * 32 : hi * 32 + 32, :]

    def second(i, slot):
        j, h, xd, t0 = rows_of(i)
        for tt in range(2):
            acc = None
            for hi in range(8):
                d = jnp.dot(w[slot, tt, hi], tab[t0 + tt, hi * 256 : hi * 256 + 256, :],
                            preferred_element_type=F32)
                acc = d if acc is None else acc + d
            stage[pl.ds(t0 + tt, 128, 8), :] = acc

    def finish(j):
        for cc in range(2):
            sb[j, cc] = stage[cc * 512 : cc * 512 + 512, :].astype(BF)

        @pl.when(j % 4 < 3)
        def _():
            for cc in range(2):
                chunk_copy(j, cc).start()

        @pl.when(j % 4 == 3)
        def _():
            partner_copy(j).start()
            own_copy(j).start()

    def pairs_of():
        live = lv[...]
        for d in range(1, NK):
            live = live + lvall[(k + d) % NK]
        return (live * (live - 1)) >> 1

    def sum_all(v):
        s = jnp.sum(jnp.sum(v, axis=0, keepdims=True), axis=1, keepdims=True)
        return jnp.broadcast_to(s, (8, LANES))

    def step(i, carry):
        slot = i % 2

        @pl.when(i <= 4)
        def _():
            table_copy((i - 1) * 2).wait()
            table_copy((i - 1) * 2 + 1).wait()

        second(i - 1, 1 - slot)
        first(i, slot)

        @pl.when(i == 4)
        def _():
            pl.semaphore_wait(bar, NK - 1 + NY - 1 + z)
            for d in range(1, NK):
                live_copy(d).start()

        @pl.when(i % 4 == 0)
        def _():
            finish(i // 4 - 1)

        @pl.when(i == 8)
        def _():
            for d in range(1, NK):
                arrival(lvall.at[(k + d) % NK], lrs.at[(k + d) % NK]).wait_recv()
            tot[...] = sum_all(pairs_of())
            for d in range(1, NY):
                y_copy(d).start()

        @pl.when(i == 12)
        def _():
            for d in range(1, NY):
                arrival(ytot.at[(y + d) % NY], yrs.at[(y + d) % NY]).wait_recv()
            sub = lax.broadcasted_iota(I32, (8, LANES), 0)
            col = jnp.where(sub == y, tot[...], 0)
            for d in range(1, NY):
                col = jnp.where(sub == (y + d) % NY, ytot[(y + d) % NY], col)
            ztot[z] = col
            for d in range(1, NZ):
                @pl.when(z - d >= 0)
                def _():
                    z_copy(-d).start()

        @pl.when(i == 20)
        def _():
            reply(1, 4)

        @pl.when(i == 26)
        def _():
            reply(4, 8)

        return carry

    first(0, 0)
    lax.fori_loop(1, 32, step, 0)
    second(31, 1)
    finish(7)

    reply(8, NZ)
    for d in range(1, NZ):
        @pl.when(z - d >= 0)
        def _():
            z_arrival(-d).wait_recv()
    lane = lax.broadcasted_iota(I32, (8, LANES), 1)
    sub = lax.broadcasted_iota(I32, (8, LANES), 0)
    before = jnp.zeros((8, LANES), I32)
    for n in range(NZ):
        earlier = jnp.logical_or(sub < y, jnp.logical_and(sub == y, n < z))
        before = before + jnp.where(earlier, ztot[n], 0)
    before = jnp.broadcast_to(jnp.sum(before, axis=0, keepdims=True), (8, LANES))
    pairs = pairs_of()
    run = pairs
    for n in range(7):
        run = run + jnp.where(lane >= (1 << n), pltpu.roll(run, 1 << n, 1), 0)
    before = before + sum_all(jnp.where(sub < k, pairs, 0))
    mine = jnp.sum(jnp.where(sub == k, run - pairs, 0), axis=0, keepdims=True)
    offs[...] = mine + before[0:1, :]

    for d in range(1, NK):
        live_copy(d).wait_send()
    for d in range(1, NZ):
        @pl.when(z + d < NZ)
        def _():
            z_copy(d).wait_send()

        @pl.when(z - d >= 0)
        def _():
            z_copy(-d).wait_send()
    for d in range(1, NY):
        y_copy(d).wait_send()
    for h in range(2):
        for j in range(3):
            for cc in range(2):
                chunk_copy(h * 4 + j, cc).wait_send()
        partner_copy(h * 4 + 3).wait_send()
        own_copy(h * 4 + 3).wait()
        for d in range(1, NK):
            src = (k + d) % NK
            arrival(out.at[h, src], rsem.at[src * 2 + h]).wait_recv()


def pool_exchange(ids, cnt, tab):
    dma = pltpu.SemaphoreType.DMA
    return pl.pallas_call(
        pool_body,
        out_shape=(jax.ShapeDtypeStruct((2, NK, 512, LANES), BF), jax.ShapeDtypeStruct((1, LANES), I32)),
        in_specs=[pl.BlockSpec(memory_space=pltpu.HBM)] * 3,
        out_specs=(pl.BlockSpec(memory_space=pltpu.HBM), pl.BlockSpec(memory_space=pltpu.VMEM)),
        scratch_shapes=[
            pltpu.VMEM((64, 1024), I32),
            pltpu.VMEM((NT, 1024), I32),
            pltpu.VMEM((NT, 2048, LANES), BF),
            pltpu.VMEM((8, NT, 4, 256), F32),
            pltpu.VMEM((8, NT, 4, 256), F32),
            pltpu.VMEM((256, 256), BF),
            pltpu.VMEM((2, 2, 8, 128, 256), BF),
            pltpu.VMEM((1024, LANES), F32),
            pltpu.VMEM((8, 2, 512, LANES), BF),
            pltpu.VMEM((8, LANES), I32),
            pltpu.VMEM((NK, 8, LANES), I32),
            pltpu.VMEM((8, LANES), I32),
            pltpu.VMEM((NY, 8, LANES), I32),
            pltpu.VMEM((NZ, 8, LANES), I32),
            dma((2,)), dma((NT,)), dma((16,)), dma((16,)), dma((2,)),
            dma((NK,)), dma((NK,)), dma((2 * NZ,)), dma((NZ,)), dma((NY,)), dma((NY,)),
        ],
        compiler_params=pltpu.CompilerParams(
            collective_id=0, has_side_effects=True, vmem_limit_bytes=60 * 2**20),
        name="pool_exchange",
    )(ids, cnt, tab)


def gram_body(src, out, g):
    low = lax.broadcasted_iota(I32, (16, LANES), 1) < 64
    for half in range(2):
        for p in range(8):
            r0 = half * 128 + p * 16
            got = [src[0, s, r0 : r0 + 16, :].astype(F32) for s in range(NK)]
            even = jnp.concatenate([v[0:8] for v in got], 0).astype(BF)
            odd = jnp.concatenate([v[8:16] for v in got], 0).astype(BF)
            for n, m in ((0, even), (1, odd)):
                full = lax.dot_general(m, jnp.concatenate([m, m], 0), TRI, preferred_element_type=F32)
                g[half, (p * 2 + n) * 64 : (p * 2 + n) * 64 + 64, :] = full
    for half in range(2):
        for i in range(32):
            lo = g[half, pl.ds(2 * i, 16, 64), :]
            hi = g[half, pl.ds(2 * i + 1, 16, 64), :]
            out[half * 16 : half * 16 + 16, i * 128 : i * 128 + 128] = jnp.where(low, lo, hi).astype(BF)


def gram(got):
    return pl.pallas_call(
        gram_body,
        grid=(4,),
        out_shape=jax.ShapeDtypeStruct((128, 4096), BF),
        in_specs=[pl.BlockSpec((1, NK, 256, LANES), lambda i: (i // 2, 0, i % 2, 0))],
        out_specs=pl.BlockSpec((32, 4096), lambda i: (i, 0)),
        scratch_shapes=[pltpu.VMEM((2, 1024, LANES), F32)],
        name="gram",
    )(got)


def body(embeddings, feature_ids, counts):
    got, offsets = pool_exchange(feature_ids.T, counts.T, embeddings)
    return gram(got), offsets.reshape(LANES)


def solution(mesh):
    return jax.shard_map(
        body, mesh=mesh,
        in_specs=(P("table", None, None), P("batch", "table"), P("batch", "table")),
        out_specs=(P(("batch", "table"), None), P(("batch", "table"))),
        check_vma=False)
```

```python
import jax
import jax.numpy as jnp
from jax import lax
from jax.experimental import pallas as pl
from jax.experimental.pallas import tpu as pltpu
from jax.sharding import PartitionSpec as P

BF = jnp.bfloat16
F32 = jnp.float32
I32 = jnp.int32
MESH = pl.DeviceIdType.MESH
MAXF = 8
NT = 8
NK = 8
NY, NZ = 4, 16
LANES = 128
TRI = (((1,), (1,)), ((), ()))


def pool_body(ids_hbm, cnt_hbm, tab_hbm, out, offs, ids, cnt, cntb, tab, ka, kb, iota, w, stage, sb, lv, lvall, tot, ytot, ztot,
              isem, tsem, ssem, rsem, lsem, lss, lrs, zss, zrs, yss, yrs):
    b, k = lax.axis_index("batch"), lax.axis_index("table")
    y, z = b // NZ, b % NZ
    x, c = k // 2, k % 2

    bar = pltpu.get_barrier_semaphore()
    for d in range(1, NK):
        pl.semaphore_signal(bar, inc=1, device_id=(b, (k + d) % NK), device_id_type=MESH)
    for d in range(1, NZ):
        @pl.when(z + d < NZ)
        def _():
            pl.semaphore_signal(bar, inc=1, device_id=(b + d, k), device_id_type=MESH)
    for d in range(1, NY):
        pl.semaphore_signal(bar, inc=1, device_id=(((y + d) % NY) * NZ + z, k), device_id_type=MESH)

    def table_copy(t):
        return pltpu.make_async_copy(tab_hbm.at[t], tab.at[t], tsem.at[t])

    id_copy = pltpu.make_async_copy(ids_hbm, ids, isem.at[0])
    count_copy = pltpu.make_async_copy(cnt_hbm, cnt, isem.at[1])
    id_copy.start()
    count_copy.start()
    for t in range(NT):
        table_copy(t).start()

    iota[...] = lax.broadcasted_iota(I32, (256, 256), 0).astype(F32).astype(BF)
    id_copy.wait()
    count_copy.wait()
    for t in range(NT):
        cntb[t] = jnp.broadcast_to(cnt[t : t + 1, :], (8, 1024))

    for q in range(8):
        on = (cnt[:, q * 128 : q * 128 + 128] > 0).astype(I32)
        lv[q : q + 1, :] = jnp.sum(on, axis=0, keepdims=True)

    def turn(j):
        return (2 + 3 * j + 3 * ((j * (j - 1)) // 2)) % 4

    def chunk_copy(j, cc):
        h, xd = j // 4, (x + turn(j % 4)) % 4
        return pltpu.make_async_remote_copy(
            src_ref=sb.at[j, cc], dst_ref=out.at[h, k], send_sem=ssem.at[j * 2 + cc],
            recv_sem=rsem.at[k * 2 + h], device_id=(b, xd * 2 + cc), device_id_type=MESH)

    def partner_copy(j):
        h = j // 4
        return pltpu.make_async_remote_copy(
            src_ref=sb.at[j, 1 - c], dst_ref=out.at[h, k], send_sem=ssem.at[j * 2],
            recv_sem=rsem.at[k * 2 + h], device_id=(b, x * 2 + 1 - c), device_id_type=MESH)

    def own_copy(j):
        h = j // 4
        return pltpu.make_async_copy(sb.at[j, c], out.at[h, k], lsem.at[h])

    def live_copy(d):
        return pltpu.make_async_remote_copy(
            src_ref=lv, dst_ref=lvall.at[k], send_sem=lss.at[d], recv_sem=lrs.at[k],
            device_id=(b, (k + d) % NK), device_id_type=MESH)

    def y_copy(d):
        return pltpu.make_async_remote_copy(
            src_ref=tot, dst_ref=ytot.at[y], send_sem=yss.at[d], recv_sem=yrs.at[y],
            device_id=(((y + d) % NY) * NZ + z, k), device_id_type=MESH)

    def z_copy(d):
        return pltpu.make_async_remote_copy(
            src_ref=ztot.at[z], dst_ref=ztot.at[z], send_sem=zss.at[d + NZ], recv_sem=zrs.at[z],
            device_id=(b + d, k), device_id_type=MESH)

    def z_arrival(d):
        return arrival(ztot.at[z + d], zrs.at[z + d])

    def reply(lo, hi):
        for d in range(lo, hi):
            @pl.when(z + d < NZ)
            def _():
                z_arrival(d).wait_recv()
                z_copy(d).start()

    def arrival(ref, sem):
        return pltpu.make_async_remote_copy(
            src_ref=ref, dst_ref=ref, send_sem=sem, recv_sem=sem, device_id=(b, k), device_id_type=MESH)

    def rows_of(i):
        j = i // 4
        return j, j // 4, (x + turn(j % 4)) % 4, (i % 4) * 2

    lane = lax.broadcasted_iota(I32, (8, LANES), 1)
    sub = lax.broadcasted_iota(I32, (8, LANES), 0)
    place = [jnp.logical_and((sub & 3) == n, (lane >> 5) == n) for n in range(4)]

    def keys(i, slot):
        j, h, xd, t0 = rows_of(i)
        for tt in range(2):
            for qq in range(2):
                c0 = pl.multiple_of((xd * 2 + qq) * LANES, LANES)
                v = ids[pl.ds(pl.multiple_of((t0 + tt) * 8, 8), 8), pl.ds(c0, LANES)]
                v = jnp.where(sub >= cntb[t0 + tt, :, pl.ds(c0, LANES)], 2048, v)
                v = jnp.where(h > 0, pltpu.roll(v, 64, 1), v)
                turned = [v] + [pltpu.roll(v, 32 * n, 1) for n in range(1, 4)]
                for a in range(2):
                    m = jnp.zeros_like(v)
                    for n in range(4):
                        m = jnp.where(place[n], turned[(n - a) % 4], m)
                    m = m + pltpu.roll(m, 7, 0)
                    m = m + pltpu.roll(m, 6, 0)
                    za = (((m >> 8) << 5) + (lane & 31)).astype(F32)
                    zb = (m & 255).astype(F32)
                    g = qq * 2 + a
                    for n in range(2):
                        ka[slot, tt, g : g + 1, n * 128 : n * 128 + 128] = za[4 * n : 4 * n + 1, :]
                        kb[slot, tt, g : g + 1, n * 128 : n * 128 + 128] = zb[4 * n : 4 * n + 1, :]

    def first(i, slot):
        one, zero = jnp.ones((16, 256), BF), jnp.zeros((16, 256), BF)
        for tt in range(2):
            for g in range(4):
                ra = jnp.broadcast_to(ka[slot, tt, g : g + 1, :], (16, 256)).astype(BF)
                rb = jnp.broadcast_to(kb[slot, tt, g : g + 1, :], (16, 256)).astype(BF)
                la, lb = [], []
                for r in range(16):
                    row = iota[r * 16 : r * 16 + 16, :]
                    la.append(jnp.where(row == ra, one, zero))
                    lb.append(jnp.where(row == rb, one, zero))
                n = lax.dot_general(jnp.concatenate(la, 0), jnp.concatenate(lb, 0), TRI,
                                    preferred_element_type=F32).astype(BF)
                for hi in range(8):
                    w[slot, tt, hi, g * 32 : g * 32 + 32, :] = n[hi * 32 : hi * 32 + 32, :]

    def second(i, slot):
        j, h, xd, t0 = rows_of(i)
        for tt in range(2):
            acc = None
            for hi in range(8):
                d = jnp.dot(w[slot, tt, hi], tab[t0 + tt, hi * 256 : hi * 256 + 256, :],
                            preferred_element_type=F32)
                acc = d if acc is None else acc + d
            stage[pl.ds(t0 + tt, 128, 8), :] = acc

    def finish(j):
        for cc in range(2):
            sb[j, cc] = stage[cc * 512 : cc * 512 + 512, :].astype(BF)

        @pl.when(j % 4 < 3)
        def _():
            for cc in range(2):
                chunk_copy(j, cc).start()

        @pl.when(j % 4 == 3)
        def _():
            partner_copy(j).start()
            own_copy(j).start()

    def pairs_of():
        live = lv[...]
        for d in range(1, NK):
            live = live + lvall[(k + d) % NK]
        return (live * (live - 1)) >> 1

    def sum_all(v):
        s = jnp.sum(jnp.sum(v, axis=0, keepdims=True), axis=1, keepdims=True)
        return jnp.broadcast_to(s, (8, LANES))

    def step(p, carry):
        i = 2 * p + 1

        @pl.when(p < 2)
        def _():
            for n in range(4):
                table_copy(p * 4 + n).wait()

        second(i - 1, 0)
        first(i, 1)
        keys(i + 1, 0)
        second(i, 1)
        first(i + 1, 0)
        keys(i + 2, 1)

        @pl.when(p == 0)
        def _():
            pl.semaphore_wait(bar, NK - 1 + NY - 1 + z)
            for d in range(1, NK):
                live_copy(d).start()

        @pl.when(p % 2 == 1)
        def _():
            finish(p // 2)

        @pl.when(p == 2)
        def _():
            for d in range(1, NK):
                arrival(lvall.at[(k + d) % NK], lrs.at[(k + d) % NK]).wait_recv()
            tot[...] = sum_all(pairs_of())
            for d in range(1, NY):
                y_copy(d).start()

        @pl.when(p == 3)
        def _():
            for d in range(1, NY):
                arrival(ytot.at[(y + d) % NY], yrs.at[(y + d) % NY]).wait_recv()
            col = jnp.where(sub == y, tot[...], 0)
            for d in range(1, NY):
                col = jnp.where(sub == (y + d) % NY, ytot[(y + d) % NY], col)
            ztot[z] = col
            for d in range(1, NZ):
                @pl.when(z - d >= 0)
                def _():
                    z_copy(-d).start()

        @pl.when(p == 8)
        def _():
            reply(1, 4)

        @pl.when(p == 11)
        def _():
            reply(4, 8)

        return carry

    keys(0, 0)
    first(0, 0)
    keys(1, 1)
    lax.fori_loop(0, 15, step, 0)
    second(30, 0)
    first(31, 1)
    second(31, 1)
    finish(7)

    reply(8, NZ)
    for d in range(1, NZ):
        @pl.when(z - d >= 0)
        def _():
            z_arrival(-d).wait_recv()
    before = jnp.zeros((8, LANES), I32)
    for n in range(NZ):
        earlier = jnp.logical_or(sub < y, jnp.logical_and(sub == y, n < z))
        before = before + jnp.where(earlier, ztot[n], 0)
    before = jnp.broadcast_to(jnp.sum(before, axis=0, keepdims=True), (8, LANES))
    pairs = pairs_of()
    run = pairs
    for n in range(7):
        run = run + jnp.where(lane >= (1 << n), pltpu.roll(run, 1 << n, 1), 0)
    before = before + sum_all(jnp.where(sub < k, pairs, 0))
    mine = jnp.sum(jnp.where(sub == k, run - pairs, 0), axis=0, keepdims=True)
    offs[...] = mine + before[0:1, :]

    for d in range(1, NK):
        live_copy(d).wait_send()
    for d in range(1, NZ):
        @pl.when(z + d < NZ)
        def _():
            z_copy(d).wait_send()

        @pl.when(z - d >= 0)
        def _():
            z_copy(-d).wait_send()
    for d in range(1, NY):
        y_copy(d).wait_send()
    for h in range(2):
        for j in range(3):
            for cc in range(2):
                chunk_copy(h * 4 + j, cc).wait_send()
        partner_copy(h * 4 + 3).wait_send()
        own_copy(h * 4 + 3).wait()
        for d in range(1, NK):
            src = (k + d) % NK
            arrival(out.at[h, src], rsem.at[src * 2 + h]).wait_recv()


def pool_exchange(ids, cnt, tab):
    dma = pltpu.SemaphoreType.DMA
    return pl.pallas_call(
        pool_body,
        out_shape=(jax.ShapeDtypeStruct((2, NK, 512, LANES), BF), jax.ShapeDtypeStruct((1, LANES), I32)),
        in_specs=[pl.BlockSpec(memory_space=pltpu.HBM)] * 3,
        out_specs=(pl.BlockSpec(memory_space=pltpu.HBM), pl.BlockSpec(memory_space=pltpu.VMEM)),
        scratch_shapes=[
            pltpu.VMEM((64, 1024), I32),
            pltpu.VMEM((NT, 1024), I32),
            pltpu.VMEM((NT, 8, 1024), I32),
            pltpu.VMEM((NT, 2048, LANES), BF),
            pltpu.VMEM((2, 2, 4, 256), F32),
            pltpu.VMEM((2, 2, 4, 256), F32),
            pltpu.VMEM((256, 256), BF),
            pltpu.VMEM((2, 2, 8, 128, 256), BF),
            pltpu.VMEM((1024, LANES), F32),
            pltpu.VMEM((8, 2, 512, LANES), BF),
            pltpu.VMEM((8, LANES), I32),
            pltpu.VMEM((NK, 8, LANES), I32),
            pltpu.VMEM((8, LANES), I32),
            pltpu.VMEM((NY, 8, LANES), I32),
            pltpu.VMEM((NZ, 8, LANES), I32),
            dma((2,)), dma((NT,)), dma((16,)), dma((16,)), dma((2,)),
            dma((NK,)), dma((NK,)), dma((2 * NZ,)), dma((NZ,)), dma((NY,)), dma((NY,)),
        ],
        compiler_params=pltpu.CompilerParams(
            collective_id=0, has_side_effects=True, vmem_limit_bytes=60 * 2**20),
        name="pool_exchange",
    )(ids, cnt, tab)


PITCH = 72


def gram_body(src, out, g):
    low = lax.broadcasted_iota(I32, (64, LANES), 1) < 64
    low8 = low[0:8]
    got = [src[0, n].astype(F32) for n in range(NK)]

    def vectors(m):
        return jnp.concatenate([v[m * 8 : m * 8 + 8] for v in got], 0)

    for m in (0, 2, 4, 6):
        four = jnp.concatenate([vectors(n) for n in (m, m + 8, m + 1, m + 9)], 0).astype(BF)
        full = lax.dot_general(four, four, TRI, preferred_element_type=F32)
        g[m * PITCH : m * PITCH + 64, :] = jnp.where(low, full[0:64, 0:128], full[64:128, 0:128])
        g[(m + 1) * PITCH : (m + 1) * PITCH + 64, :] = jnp.where(low, full[128:192, 128:], full[192:256, 128:])
    for i in range(32):
        even = g[pl.ds(2 * i, 8, PITCH), :]
        odd = g[pl.ds(2 * i + 1, 8, PITCH), :]
        a = jnp.where(low8, even, pltpu.roll(odd, 64, 1))
        b = jnp.where(low8, pltpu.roll(even, 64, 1), odd)
        out[:, i * 128 : i * 128 + 128] = jnp.concatenate([a, b], 0).astype(BF)


def gram(got):
    return pl.pallas_call(
        gram_body,
        grid=(8,),
        out_shape=jax.ShapeDtypeStruct((128, 4096), BF),
        in_specs=[pl.BlockSpec((1, NK, 128, LANES), lambda i: (i // 4, 0, i % 4, 0))],
        out_specs=pl.BlockSpec((16, 4096), lambda i: (i, 0)),
        scratch_shapes=[pltpu.VMEM((8 * PITCH, LANES), F32)],
        name="gram",
    )(got)


def body(embeddings, feature_ids, counts):
    got, offsets = pool_exchange(feature_ids.T, counts.T, embeddings)
    return gram(got), offsets.reshape(LANES)


def solution(mesh):
    return jax.shard_map(
        body, mesh=mesh,
        in_specs=(P("table", None, None), P("batch", "table"), P("batch", "table")),
        out_specs=(P(("batch", "table"), None), P(("batch", "table"))),
        check_vma=False)
```

```python
import jax
import jax.numpy as jnp
from jax import lax
from jax.experimental import pallas as pl
from jax.experimental.pallas import tpu as pltpu
from jax.sharding import PartitionSpec as P

BF = jnp.bfloat16
F32 = jnp.float32
I32 = jnp.int32
MESH = pl.DeviceIdType.MESH
MAXF = 8
NT = 8
NK = 8
NY, NZ = 4, 16
LANES = 128
RANK = (0, 1, 2, 3, 4, 5, 6, 7, 8, 10, 12, 14, 15, 13, 11, 9)
TRI = (((1,), (1,)), ((), ()))


def pool_body(ids_hbm, cnt_hbm, tab_hbm, out, offs, ids, cnt, cntb, tab, ka, kb, iota, w, stage, sb, lv, lvall, tot, ytot, ztot,
              isem, tsem, ssem, rsem, lsem, lss, lrs, zss, zrs, yss, yrs):
    b, k = lax.axis_index("batch"), lax.axis_index("table")
    y, z = b // NZ, b % NZ
    x, c = k // 2, k % 2
    rank = sum(r * (1 - ((z - n) * (z - n) + 255) // 256) for n, r in enumerate(RANK))

    bar = pltpu.get_barrier_semaphore()
    for d in range(1, NK):
        pl.semaphore_signal(bar, inc=1, device_id=(b, (k + d) % NK), device_id_type=MESH)
    for n in range(NZ):
        @pl.when(RANK[n] > rank)
        def _():
            pl.semaphore_signal(bar, inc=1, device_id=(y * NZ + n, k), device_id_type=MESH)
    for d in range(1, NY):
        pl.semaphore_signal(bar, inc=1, device_id=(((y + d) % NY) * NZ + z, k), device_id_type=MESH)

    def table_copy(t):
        return pltpu.make_async_copy(tab_hbm.at[t], tab.at[t], tsem.at[t])

    id_copy = pltpu.make_async_copy(ids_hbm, ids, isem.at[0])
    count_copy = pltpu.make_async_copy(cnt_hbm, cnt, isem.at[1])
    id_copy.start()
    count_copy.start()
    for t in range(NT):
        table_copy(t).start()

    iota[...] = lax.broadcasted_iota(I32, (256, 256), 0).astype(F32).astype(BF)
    id_copy.wait()
    count_copy.wait()
    for t in range(NT):
        cntb[t] = jnp.broadcast_to(cnt[t : t + 1, :], (8, 1024))

    for q in range(8):
        on = (cnt[:, q * 128 : q * 128 + 128] > 0).astype(I32)
        lv[q : q + 1, :] = jnp.sum(on, axis=0, keepdims=True)

    def turn(j):
        return (2 + 3 * j + 3 * ((j * (j - 1)) // 2)) % 4

    def chunk_copy(j, cc):
        h, xd = j // 4, (x + turn(j % 4)) % 4
        return pltpu.make_async_remote_copy(
            src_ref=sb.at[j, cc], dst_ref=out.at[h, k], send_sem=ssem.at[j * 2 + cc],
            recv_sem=rsem.at[k * 2 + h], device_id=(b, xd * 2 + cc), device_id_type=MESH)

    def partner_copy(j):
        h = j // 4
        return pltpu.make_async_remote_copy(
            src_ref=sb.at[j, 1 - c], dst_ref=out.at[h, k], send_sem=ssem.at[j * 2],
            recv_sem=rsem.at[k * 2 + h], device_id=(b, x * 2 + 1 - c), device_id_type=MESH)

    def own_copy(j):
        h = j // 4
        return pltpu.make_async_copy(sb.at[j, c], out.at[h, k], lsem.at[h])

    def live_copy(d):
        return pltpu.make_async_remote_copy(
            src_ref=lv, dst_ref=lvall.at[k], send_sem=lss.at[d], recv_sem=lrs.at[k],
            device_id=(b, (k + d) % NK), device_id_type=MESH)

    def y_copy(d):
        return pltpu.make_async_remote_copy(
            src_ref=tot, dst_ref=ytot.at[y], send_sem=yss.at[d], recv_sem=yrs.at[y],
            device_id=(((y + d) % NY) * NZ + z, k), device_id_type=MESH)

    def z_copy(n):
        return pltpu.make_async_remote_copy(
            src_ref=ztot.at[z], dst_ref=ztot.at[z], send_sem=zss.at[n], recv_sem=zrs.at[z],
            device_id=(y * NZ + n, k), device_id_type=MESH)

    def z_arrival(n):
        return arrival(ztot.at[n], zrs.at[n])

    def reply(lo, hi):
        for n in range(NZ):
            @pl.when(jnp.logical_and(RANK[n] - rank >= lo, RANK[n] - rank < hi))
            def _():
                z_arrival(n).wait_recv()
                z_copy(n).start()

    def arrival(ref, sem):
        return pltpu.make_async_remote_copy(
            src_ref=ref, dst_ref=ref, send_sem=sem, recv_sem=sem, device_id=(b, k), device_id_type=MESH)

    def rows_of(i):
        j = i // 4
        return j, j // 4, (x + turn(j % 4)) % 4, (i % 4) * 2

    lane = lax.broadcasted_iota(I32, (8, LANES), 1)
    sub = lax.broadcasted_iota(I32, (8, LANES), 0)
    place = [jnp.logical_and((sub & 3) == n, (lane >> 5) == n) for n in range(4)]

    def keys(i, slot):
        j, h, xd, t0 = rows_of(i)
        for tt in range(2):
            for qq in range(2):
                c0 = pl.multiple_of((xd * 2 + qq) * LANES, LANES)
                v = ids[pl.ds(pl.multiple_of((t0 + tt) * 8, 8), 8), pl.ds(c0, LANES)]
                v = jnp.where(sub >= cntb[t0 + tt, :, pl.ds(c0, LANES)], 2048, v)
                v = jnp.where(h > 0, pltpu.roll(v, 64, 1), v)
                turned = [v] + [pltpu.roll(v, 32 * n, 1) for n in range(1, 4)]
                for a in range(2):
                    m = jnp.zeros_like(v)
                    for n in range(4):
                        m = jnp.where(place[n], turned[(n - a) % 4], m)
                    m = m + pltpu.roll(m, 7, 0)
                    m = m + pltpu.roll(m, 6, 0)
                    za = (((m >> 8) << 5) + (lane & 31)).astype(F32)
                    zb = (m & 255).astype(F32)
                    g = qq * 2 + a
                    for n in range(2):
                        ka[slot, tt, g : g + 1, n * 128 : n * 128 + 128] = za[4 * n : 4 * n + 1, :]
                        kb[slot, tt, g : g + 1, n * 128 : n * 128 + 128] = zb[4 * n : 4 * n + 1, :]

    def first(i, slot):
        one, zero = jnp.ones((16, 256), BF), jnp.zeros((16, 256), BF)
        for tt in range(2):
            for g in range(4):
                ra = jnp.broadcast_to(ka[slot, tt, g : g + 1, :], (16, 256)).astype(BF)
                rb = jnp.broadcast_to(kb[slot, tt, g : g + 1, :], (16, 256)).astype(BF)
                la, lb = [], []
                for r in range(16):
                    row = iota[r * 16 : r * 16 + 16, :]
                    la.append(jnp.where(row == ra, one, zero))
                    lb.append(jnp.where(row == rb, one, zero))
                n = lax.dot_general(jnp.concatenate(la, 0), jnp.concatenate(lb, 0), TRI,
                                    preferred_element_type=F32).astype(BF)
                for hi in range(8):
                    w[slot, tt, hi, g * 32 : g * 32 + 32, :] = n[hi * 32 : hi * 32 + 32, :]

    def second(i, slot):
        j, h, xd, t0 = rows_of(i)
        for tt in range(2):
            acc = None
            for hi in range(8):
                d = jnp.dot(w[slot, tt, hi], tab[t0 + tt, hi * 256 : hi * 256 + 256, :],
                            preferred_element_type=F32)
                acc = d if acc is None else acc + d
            stage[pl.ds(t0 + tt, 128, 8), :] = acc

    def finish(j):
        for cc in range(2):
            sb[j, cc] = stage[cc * 512 : cc * 512 + 512, :].astype(BF)

        @pl.when(j % 4 < 3)
        def _():
            for cc in range(2):
                chunk_copy(j, cc).start()

        @pl.when(j % 4 == 3)
        def _():
            partner_copy(j).start()
            own_copy(j).start()

    def pairs_of():
        live = lv[...]
        for d in range(1, NK):
            live = live + lvall[(k + d) % NK]
        return (live * (live - 1)) >> 1

    def sum_all(v):
        s = jnp.sum(jnp.sum(v, axis=0, keepdims=True), axis=1, keepdims=True)
        return jnp.broadcast_to(s, (8, LANES))

    def step(p, carry):
        i = 2 * p + 1

        @pl.when(p < 2)
        def _():
            for n in range(4):
                table_copy(p * 4 + n).wait()

        second(i - 1, 0)
        first(i, 1)
        keys(i + 1, 0)
        second(i, 1)
        first(i + 1, 0)
        keys(i + 2, 1)

        @pl.when(p == 0)
        def _():
            pl.semaphore_wait(bar, NK - 1 + NY - 1 + rank)
            for d in range(1, NK):
                live_copy(d).start()

        @pl.when(p % 2 == 1)
        def _():
            finish(p // 2)

        @pl.when(p == 2)
        def _():
            for d in range(1, NK):
                arrival(lvall.at[(k + d) % NK], lrs.at[(k + d) % NK]).wait_recv()
            tot[...] = sum_all(pairs_of())
            for d in range(1, NY):
                y_copy(d).start()

        @pl.when(p == 3)
        def _():
            for d in range(1, NY):
                arrival(ytot.at[(y + d) % NY], yrs.at[(y + d) % NY]).wait_recv()
            col = jnp.where(sub == y, tot[...], 0)
            for d in range(1, NY):
                col = jnp.where(sub == (y + d) % NY, ytot[(y + d) % NY], col)
            ztot[z] = col
            for n in range(NZ):
                @pl.when(RANK[n] < rank)
                def _():
                    z_copy(n).start()

        @pl.when(p == 8)
        def _():
            reply(1, 4)

        @pl.when(p == 11)
        def _():
            reply(4, 8)

        return carry

    keys(0, 0)
    first(0, 0)
    keys(1, 1)
    lax.fori_loop(0, 15, step, 0)
    second(30, 0)
    first(31, 1)
    second(31, 1)
    finish(7)

    reply(8, NZ)
    for n in range(NZ):
        @pl.when(RANK[n] < rank)
        def _():
            z_arrival(n).wait_recv()
    before = jnp.zeros((8, LANES), I32)
    for n in range(NZ):
        earlier = jnp.logical_or(sub < y, jnp.logical_and(sub == y, n < z))
        before = before + jnp.where(earlier, ztot[n], 0)
    before = jnp.broadcast_to(jnp.sum(before, axis=0, keepdims=True), (8, LANES))
    pairs = pairs_of()
    run = pairs
    for n in range(7):
        run = run + jnp.where(lane >= (1 << n), pltpu.roll(run, 1 << n, 1), 0)
    before = before + sum_all(jnp.where(sub < k, pairs, 0))
    mine = jnp.sum(jnp.where(sub == k, run - pairs, 0), axis=0, keepdims=True)
    offs[...] = mine + before[0:1, :]

    for d in range(1, NK):
        live_copy(d).wait_send()
    for n in range(NZ):
        @pl.when(RANK[n] != rank)
        def _():
            z_copy(n).wait_send()
    for d in range(1, NY):
        y_copy(d).wait_send()
    for h in range(2):
        for j in range(3):
            for cc in range(2):
                chunk_copy(h * 4 + j, cc).wait_send()
        partner_copy(h * 4 + 3).wait_send()
        own_copy(h * 4 + 3).wait()
        for d in range(1, NK):
            src = (k + d) % NK
            arrival(out.at[h, src], rsem.at[src * 2 + h]).wait_recv()


def pool_exchange(ids, cnt, tab):
    dma = pltpu.SemaphoreType.DMA
    return pl.pallas_call(
        pool_body,
        out_shape=(jax.ShapeDtypeStruct((2, NK, 512, LANES), BF), jax.ShapeDtypeStruct((1, LANES), I32)),
        in_specs=[pl.BlockSpec(memory_space=pltpu.HBM)] * 3,
        out_specs=(pl.BlockSpec(memory_space=pltpu.HBM), pl.BlockSpec(memory_space=pltpu.VMEM)),
        scratch_shapes=[
            pltpu.VMEM((64, 1024), I32),
            pltpu.VMEM((NT, 1024), I32),
            pltpu.VMEM((NT, 8, 1024), I32),
            pltpu.VMEM((NT, 2048, LANES), BF),
            pltpu.VMEM((2, 2, 4, 256), F32),
            pltpu.VMEM((2, 2, 4, 256), F32),
            pltpu.VMEM((256, 256), BF),
            pltpu.VMEM((2, 2, 8, 128, 256), BF),
            pltpu.VMEM((1024, LANES), F32),
            pltpu.VMEM((8, 2, 512, LANES), BF),
            pltpu.VMEM((8, LANES), I32),
            pltpu.VMEM((NK, 8, LANES), I32),
            pltpu.VMEM((8, LANES), I32),
            pltpu.VMEM((NY, 8, LANES), I32),
            pltpu.VMEM((NZ, 8, LANES), I32),
            dma((2,)), dma((NT,)), dma((16,)), dma((16,)), dma((2,)),
            dma((NK,)), dma((NK,)), dma((NZ,)), dma((NZ,)), dma((NY,)), dma((NY,)),
        ],
        compiler_params=pltpu.CompilerParams(
            collective_id=0, has_side_effects=True, vmem_limit_bytes=60 * 2**20),
        name="pool_exchange",
    )(ids, cnt, tab)


PITCH = 72


def gram_body(src, out, buf, res, g, isem, osem):
    low = lax.broadcasted_iota(I32, (64, LANES), 1) < 64
    low8 = low[0:8]

    def load(n):
        return pltpu.make_async_copy(
            src.at[n // 2, :, pl.ds(pl.multiple_of((n % 2) * 256, 256), 256)], buf.at[n], isem.at[n])

    def store(n):
        return pltpu.make_async_copy(
            res.at[n], out.at[pl.ds(pl.multiple_of(n * 32, 32), 32)], osem.at[n])

    for n in range(4):
        load(n).start()

    def part(n, carry):
        load(n).wait()
        for half in range(2):
            got = [buf[n, v, half * 128 : half * 128 + 128].astype(F32) for v in range(NK)]

            def vectors(m):
                return jnp.concatenate([v[m * 8 : m * 8 + 8] for v in got], 0)

            for m in (0, 2, 4, 6):
                four = jnp.concatenate([vectors(r) for r in (m, m + 8, m + 1, m + 9)], 0).astype(BF)
                full = lax.dot_general(four, four, TRI, preferred_element_type=F32)
                g[half, m * PITCH : m * PITCH + 64, :] = jnp.where(low, full[0:64, 0:128], full[64:128, 0:128])
                g[half, (m + 1) * PITCH : (m + 1) * PITCH + 64, :] = jnp.where(
                    low, full[128:192, 128:], full[192:256, 128:])
        for half in range(2):
            for i in range(32):
                even = g[half, pl.ds(2 * i, 8, PITCH), :]
                odd = g[half, pl.ds(2 * i + 1, 8, PITCH), :]
                a = jnp.where(low8, even, pltpu.roll(odd, 64, 1))
                b = jnp.where(low8, pltpu.roll(even, 64, 1), odd)
                res[n, half * 16 : half * 16 + 16, i * 128 : i * 128 + 128] = jnp.concatenate([a, b], 0).astype(BF)
        store(n).start()
        return carry

    lax.fori_loop(0, 4, part, 0)
    for n in range(4):
        store(n).wait()


def gram(got):
    return pl.pallas_call(
        gram_body,
        out_shape=jax.ShapeDtypeStruct((128, 4096), BF),
        in_specs=[pl.BlockSpec(memory_space=pltpu.HBM)],
        out_specs=pl.BlockSpec(memory_space=pltpu.HBM),
        scratch_shapes=[
            pltpu.VMEM((4, NK, 256, LANES), BF),
            pltpu.VMEM((4, 32, 4096), BF),
            pltpu.VMEM((2, 8 * PITCH, LANES), F32),
            pltpu.SemaphoreType.DMA((4,)),
            pltpu.SemaphoreType.DMA((4,)),
        ],
        name="gram",
    )(got)


def body(embeddings, feature_ids, counts):
    got, offsets = pool_exchange(feature_ids.T, counts.T, embeddings)
    return gram(got), offsets.reshape(LANES)


def solution(mesh):
    return jax.shard_map(
        body, mesh=mesh,
        in_specs=(P("table", None, None), P("batch", "table"), P("batch", "table")),
        out_specs=(P(("batch", "table"), None), P(("batch", "table"))),
        check_vma=False)
```

```python
import jax
import jax.numpy as jnp
from jax import lax
from jax.experimental import pallas as pl
from jax.experimental.pallas import tpu as pltpu
from jax.sharding import PartitionSpec as P

BF = jnp.bfloat16
F8 = jnp.float8_e4m3fn
F32 = jnp.float32
I32 = jnp.int32
MESH = pl.DeviceIdType.MESH
MAXF = 8
NT = 8
NK = 8
NY, NZ = 4, 16
LANES = 128
RANK = (0, 1, 2, 3, 4, 5, 6, 7, 8, 10, 12, 15, 14, 13, 11, 9)
TRI = (((1,), (1,)), ((), ()))


def pool_body(ids_hbm, cnt_hbm, tab_hbm, out, offs, ids, cnt, cntb, tab, ka, kb, iota, w, stage, sb, lv, lvall, tot, ytot, ztot,
              isem, tsem, ssem, rsem, lsem, lss, lrs, zss, zrs, yss, yrs):
    b, k = lax.axis_index("batch"), lax.axis_index("table")
    y, z = b // NZ, b % NZ
    x, c = k // 2, k % 2
    rank = sum(r * (1 - ((z - n) * (z - n) + 255) // 256) for n, r in enumerate(RANK))

    bar = pltpu.get_barrier_semaphore()
    for d in range(1, NK):
        pl.semaphore_signal(bar, inc=1, device_id=(b, (k + d) % NK), device_id_type=MESH)
    for n in range(NZ):
        @pl.when(RANK[n] > rank)
        def _():
            pl.semaphore_signal(bar, inc=1, device_id=(y * NZ + n, k), device_id_type=MESH)
    for d in range(1, NY):
        pl.semaphore_signal(bar, inc=1, device_id=(((y + d) % NY) * NZ + z, k), device_id_type=MESH)

    def table_copy(t):
        return pltpu.make_async_copy(tab_hbm.at[t], tab.at[t], tsem.at[t])

    id_copy = pltpu.make_async_copy(ids_hbm, ids, isem.at[0])
    count_copy = pltpu.make_async_copy(cnt_hbm, cnt, isem.at[1])
    id_copy.start()
    count_copy.start()
    for t in range(NT):
        table_copy(t).start()

    iota[...] = lax.broadcasted_iota(I32, (256, 256), 0).astype(F32).astype(BF)
    id_copy.wait()
    count_copy.wait()
    for t in range(NT):
        cntb[t] = jnp.broadcast_to(cnt[t : t + 1, :], (8, 1024))

    for q in range(8):
        on = (cnt[:, q * 128 : q * 128 + 128] > 0).astype(I32)
        lv[q : q + 1, :] = jnp.sum(on, axis=0, keepdims=True)

    def turn(j):
        return (2 + 3 * j + 3 * ((j * (j - 1)) // 2)) % 4

    def chunk_copy(j, cc):
        h, xd = j // 4, (x + turn(j % 4)) % 4
        return pltpu.make_async_remote_copy(
            src_ref=sb.at[j, cc], dst_ref=out.at[h, k], send_sem=ssem.at[j * 2 + cc],
            recv_sem=rsem.at[k * 2 + h], device_id=(b, xd * 2 + cc), device_id_type=MESH)

    def partner_copy(j):
        h = j // 4
        return pltpu.make_async_remote_copy(
            src_ref=sb.at[j, 1 - c], dst_ref=out.at[h, k], send_sem=ssem.at[j * 2],
            recv_sem=rsem.at[k * 2 + h], device_id=(b, x * 2 + 1 - c), device_id_type=MESH)

    def own_copy(j):
        h = j // 4
        return pltpu.make_async_copy(sb.at[j, c], out.at[h, k], lsem.at[h])

    def live_copy(d):
        return pltpu.make_async_remote_copy(
            src_ref=lv, dst_ref=lvall.at[k], send_sem=lss.at[d], recv_sem=lrs.at[k],
            device_id=(b, (k + d) % NK), device_id_type=MESH)

    def y_copy(d):
        return pltpu.make_async_remote_copy(
            src_ref=tot, dst_ref=ytot.at[y], send_sem=yss.at[d], recv_sem=yrs.at[y],
            device_id=(((y + d) % NY) * NZ + z, k), device_id_type=MESH)

    def z_copy(n):
        return pltpu.make_async_remote_copy(
            src_ref=ztot.at[z], dst_ref=ztot.at[z], send_sem=zss.at[n], recv_sem=zrs.at[z],
            device_id=(y * NZ + n, k), device_id_type=MESH)

    def z_arrival(n):
        return arrival(ztot.at[n], zrs.at[n])

    def reply(lo, hi):
        for n in range(NZ):
            @pl.when(jnp.logical_and(RANK[n] - rank >= lo, RANK[n] - rank < hi))
            def _():
                z_arrival(n).wait_recv()
                z_copy(n).start()

    def arrival(ref, sem):
        return pltpu.make_async_remote_copy(
            src_ref=ref, dst_ref=ref, send_sem=sem, recv_sem=sem, device_id=(b, k), device_id_type=MESH)

    def rows_of(i):
        j = i // 4
        return j, j // 4, (x + turn(j % 4)) % 4, (i % 4) * 2

    lane = lax.broadcasted_iota(I32, (8, LANES), 1)
    sub = lax.broadcasted_iota(I32, (8, LANES), 0)
    place = [jnp.logical_and((sub & 3) == n, (lane >> 5) == n) for n in range(4)]

    def keys(i, slot):
        j, h, xd, t0 = rows_of(i)
        for tt in range(2):
            for qq in range(2):
                c0 = pl.multiple_of((xd * 2 + qq) * LANES, LANES)
                v = ids[pl.ds(pl.multiple_of((t0 + tt) * 8, 8), 8), pl.ds(c0, LANES)]
                v = jnp.where(sub >= cntb[t0 + tt, :, pl.ds(c0, LANES)], 2048, v)
                v = jnp.where(h > 0, pltpu.roll(v, 64, 1), v)
                turned = [v] + [pltpu.roll(v, 32 * n, 1) for n in range(1, 4)]
                for a in range(2):
                    m = jnp.zeros_like(v)
                    for n in range(4):
                        m = jnp.where(place[n], turned[(n - a) % 4], m)
                    m = m + pltpu.roll(m, 7, 0)
                    m = m + pltpu.roll(m, 6, 0)
                    za = (((m >> 8) << 5) + (lane & 31)).astype(F32)
                    zb = (m & 255).astype(F32)
                    g = qq * 2 + a
                    for n in range(2):
                        ka[slot, tt, g : g + 1, n * 128 : n * 128 + 128] = za[4 * n : 4 * n + 1, :]
                        kb[slot, tt, g : g + 1, n * 128 : n * 128 + 128] = zb[4 * n : 4 * n + 1, :]

    def first(i, slot):
        one, zero = jnp.ones((16, 256), BF), jnp.zeros((16, 256), BF)
        for tt in range(2):
            for g in range(4):
                ra = jnp.broadcast_to(ka[slot, tt, g : g + 1, :], (16, 256)).astype(BF)
                rb = jnp.broadcast_to(kb[slot, tt, g : g + 1, :], (16, 256)).astype(BF)
                la, lb = [], []
                for r in range(16):
                    row = iota[r * 16 : r * 16 + 16, :]
                    la.append(jnp.where(row == ra, one, zero))
                    lb.append(jnp.where(row == rb, one, zero))
                n = lax.dot_general(jnp.concatenate(la, 0).astype(F8), jnp.concatenate(lb, 0).astype(F8), TRI,
                                    preferred_element_type=F32).astype(BF)
                for hi in range(8):
                    w[slot, tt, hi, g * 32 : g * 32 + 32, :] = n[hi * 32 : hi * 32 + 32, :]

    def second(i, slot):
        j, h, xd, t0 = rows_of(i)
        for tt in range(2):
            acc = None
            for hi in range(8):
                d = jnp.dot(w[slot, tt, hi], tab[t0 + tt, hi * 256 : hi * 256 + 256, :],
                            preferred_element_type=F32)
                acc = d if acc is None else acc + d
            stage[pl.ds(t0 + tt, 128, 8), :] = acc

    def finish(j):
        for cc in range(2):
            sb[j, cc] = stage[cc * 512 : cc * 512 + 512, :].astype(BF)

        @pl.when(j % 4 < 3)
        def _():
            for cc in range(2):
                chunk_copy(j, cc).start()

        @pl.when(j % 4 == 3)
        def _():
            partner_copy(j).start()
            own_copy(j).start()

    def pairs_of():
        live = lv[...]
        for d in range(1, NK):
            live = live + lvall[(k + d) % NK]
        return (live * (live - 1)) >> 1

    def sum_all(v):
        s = jnp.sum(jnp.sum(v, axis=0, keepdims=True), axis=1, keepdims=True)
        return jnp.broadcast_to(s, (8, LANES))

    def step(p, carry):
        i = 2 * p + 1

        @pl.when(p < 2)
        def _():
            for n in range(4):
                table_copy(p * 4 + n).wait()

        second(i - 1, 0)
        first(i, 1)
        keys(i + 1, 0)
        second(i, 1)
        first(i + 1, 0)
        keys(i + 2, 1)

        @pl.when(p == 1)
        def _():
            pl.semaphore_wait(bar, NK - 1 + NY - 1 + rank)
            for d in range(1, NK):
                live_copy(d).start()

        @pl.when(p % 2 == 1)
        def _():
            finish(p // 2)

        @pl.when(p == 3)
        def _():
            for d in range(1, NK):
                arrival(lvall.at[(k + d) % NK], lrs.at[(k + d) % NK]).wait_recv()
            tot[...] = sum_all(pairs_of())
            for d in range(1, NY):
                y_copy(d).start()

        @pl.when(p == 4)
        def _():
            for d in range(1, NY):
                arrival(ytot.at[(y + d) % NY], yrs.at[(y + d) % NY]).wait_recv()
            col = jnp.where(sub == y, tot[...], 0)
            for d in range(1, NY):
                col = jnp.where(sub == (y + d) % NY, ytot[(y + d) % NY], col)
            ztot[z] = col
            for n in range(NZ):
                @pl.when(RANK[n] < rank)
                def _():
                    z_copy(n).start()

        @pl.when(p == 9)
        def _():
            reply(1, 4)

        @pl.when(p == 12)
        def _():
            reply(4, 8)

        return carry

    keys(0, 0)
    first(0, 0)
    keys(1, 1)
    lax.fori_loop(0, 15, step, 0)
    second(30, 0)
    first(31, 1)
    second(31, 1)
    finish(7)

    reply(8, NZ)
    for n in range(NZ):
        @pl.when(RANK[n] < rank)
        def _():
            z_arrival(n).wait_recv()
    before = jnp.zeros((8, LANES), I32)
    for n in range(NZ):
        earlier = jnp.logical_or(sub < y, jnp.logical_and(sub == y, n < z))
        before = before + jnp.where(earlier, ztot[n], 0)
    before = jnp.broadcast_to(jnp.sum(before, axis=0, keepdims=True), (8, LANES))
    pairs = pairs_of()
    run = pairs
    for n in range(7):
        run = run + jnp.where(lane >= (1 << n), pltpu.roll(run, 1 << n, 1), 0)
    before = before + sum_all(jnp.where(sub < k, pairs, 0))
    mine = jnp.sum(jnp.where(sub == k, run - pairs, 0), axis=0, keepdims=True)
    offs[...] = mine + before[0:1, :]

    for d in range(1, NK):
        live_copy(d).wait_send()
    for n in range(NZ):
        @pl.when(RANK[n] != rank)
        def _():
            z_copy(n).wait_send()
    for d in range(1, NY):
        y_copy(d).wait_send()
    for h in range(2):
        for j in range(3):
            for cc in range(2):
                chunk_copy(h * 4 + j, cc).wait_send()
        partner_copy(h * 4 + 3).wait_send()
        own_copy(h * 4 + 3).wait()
        for d in range(1, NK):
            src = (k + d) % NK
            arrival(out.at[h, src], rsem.at[src * 2 + h]).wait_recv()


def pool_exchange(ids, cnt, tab):
    dma = pltpu.SemaphoreType.DMA
    return pl.pallas_call(
        pool_body,
        out_shape=(jax.ShapeDtypeStruct((2, NK, 512, LANES), BF), jax.ShapeDtypeStruct((1, LANES), I32)),
        in_specs=[pl.BlockSpec(memory_space=pltpu.HBM)] * 3,
        out_specs=(pl.BlockSpec(memory_space=pltpu.HBM), pl.BlockSpec(memory_space=pltpu.VMEM)),
        scratch_shapes=[
            pltpu.VMEM((64, 1024), I32),
            pltpu.VMEM((NT, 1024), I32),
            pltpu.VMEM((NT, 8, 1024), I32),
            pltpu.VMEM((NT, 2048, LANES), BF),
            pltpu.VMEM((2, 2, 4, 256), F32),
            pltpu.VMEM((2, 2, 4, 256), F32),
            pltpu.VMEM((256, 256), BF),
            pltpu.VMEM((2, 2, 8, 128, 256), BF),
            pltpu.VMEM((1024, LANES), F32),
            pltpu.VMEM((8, 2, 512, LANES), BF),
            pltpu.VMEM((8, LANES), I32),
            pltpu.VMEM((NK, 8, LANES), I32),
            pltpu.VMEM((8, LANES), I32),
            pltpu.VMEM((NY, 8, LANES), I32),
            pltpu.VMEM((NZ, 8, LANES), I32),
            dma((2,)), dma((NT,)), dma((16,)), dma((16,)), dma((2,)),
            dma((NK,)), dma((NK,)), dma((NZ,)), dma((NZ,)), dma((NY,)), dma((NY,)),
        ],
        compiler_params=pltpu.CompilerParams(
            collective_id=0, has_side_effects=True, vmem_limit_bytes=60 * 2**20),
        name="pool_exchange",
    )(ids, cnt, tab)


PITCH = 72


def gram_body(src, out, buf, res, g, isem, osem):
    low = lax.broadcasted_iota(I32, (64, LANES), 1) < 64
    low8 = low[0:8]

    def load(n):
        return pltpu.make_async_copy(
            src.at[n // 2, :, pl.ds(pl.multiple_of((n % 2) * 256, 256), 256)], buf.at[n], isem.at[n])

    def store(n):
        return pltpu.make_async_copy(
            res.at[n], out.at[pl.ds(pl.multiple_of(n * 32, 32), 32)], osem.at[n])

    for n in range(4):
        load(n).start()

    def part(n, carry):
        load(n).wait()
        for half in range(2):
            got = [buf[n, v, half * 128 : half * 128 + 128].astype(F32) for v in range(NK)]

            def vectors(m):
                return jnp.concatenate([v[m * 8 : m * 8 + 8] for v in got], 0)

            for m in (0, 2, 4, 6):
                four = jnp.concatenate([vectors(r) for r in (m, m + 8, m + 1, m + 9)], 0).astype(BF)
                full = lax.dot_general(four, four, TRI, preferred_element_type=F32)
                g[half, m * PITCH : m * PITCH + 64, :] = jnp.where(low, full[0:64, 0:128], full[64:128, 0:128])
                g[half, (m + 1) * PITCH : (m + 1) * PITCH + 64, :] = jnp.where(
                    low, full[128:192, 128:], full[192:256, 128:])
        for half in range(2):
            for i in range(32):
                even = g[half, pl.ds(2 * i, 8, PITCH), :]
                odd = g[half, pl.ds(2 * i + 1, 8, PITCH), :]
                a = jnp.where(low8, even, pltpu.roll(odd, 64, 1))
                b = jnp.where(low8, pltpu.roll(even, 64, 1), odd)
                res[n, half * 16 : half * 16 + 16, i * 128 : i * 128 + 128] = jnp.concatenate([a, b], 0).astype(BF)
        store(n).start()
        return carry

    lax.fori_loop(0, 4, part, 0)
    for n in range(4):
        store(n).wait()


def gram(got):
    return pl.pallas_call(
        gram_body,
        out_shape=jax.ShapeDtypeStruct((128, 4096), BF),
        in_specs=[pl.BlockSpec(memory_space=pltpu.HBM)],
        out_specs=pl.BlockSpec(memory_space=pltpu.HBM),
        scratch_shapes=[
            pltpu.VMEM((4, NK, 256, LANES), BF),
            pltpu.VMEM((4, 32, 4096), BF),
            pltpu.VMEM((2, 8 * PITCH, LANES), F32),
            pltpu.SemaphoreType.DMA((4,)),
            pltpu.SemaphoreType.DMA((4,)),
        ],
        name="gram",
    )(got)


def body(embeddings, feature_ids, counts):
    got, offsets = pool_exchange(feature_ids.T, counts.T, embeddings)
    return gram(got), offsets.reshape(LANES)


def solution(mesh):
    return jax.shard_map(
        body, mesh=mesh,
        in_specs=(P("table", None, None), P("batch", "table"), P("batch", "table")),
        out_specs=(P(("batch", "table"), None), P(("batch", "table"))),
        check_vma=False)
```
